128 devices in a mesh: pts: 8 (over x_hi, y), med: 16 (over x_lo, z, core).
Axes of the slice: x: 4 (x_hi: 2, x_lo: 2; x = x_hi * 2 + x_lo), y: 4, z: 4, core: 2. Of those that a mesh axis runs over, the one named last changes fastest.
Arguments:
- points: float32 [262144, 1024], P(('pts', 'med')), may hold values from -6 to 6
- weights: float32 [262144], P(('pts', 'med')), may hold values from 0.2 to 6
- medoid_ids: int32 [2048], replicated, may hold values from 0 to 262143, as said below
Outputs:
- cover: float32 [262144], P(('pts', 'med'))
- total: float32 [], replicated
The draws below stay inside these ranges and needn't reach their ends.
Inputs may be any that keep to these rules, and one draw needn't show every extreme that they name: `medoid_ids`: distinct row numbers; the points of one device hold at most 24 medoids, and some device holds exactly 24 in every draw.
All inputs are finite; a program needn't handle non-finite values.
Results may differ from the reference program's by a relative error of at most 0.00005.
Values sent between devices are 32-bit elements; how exact they have to be, the bound alone decides.
No kernel may reach another device: no remote copies, remote signals or barrier semaphores. Data moves between devices by JAX's collectives and lax.ppermute only.
A program may use at most 128 MiB of HBM per device.

```python
import jax
import jax.numpy as jnp
from jax import lax

D = 1024
ROWS_DEV = 2048
CAP = 24
POINTS = 262144
MEDOIDS = 2048
N_PTS = 8
N_MED = 16


def draw_medoid_ids(key, part):
    devcount = N_PTS * N_MED
    slots = devcount * CAP
    key_rank = jax.random.fold_in(key, 31)
    key_forced = jax.random.fold_in(key, 32)
    key_rows = jax.random.fold_in(key, 33)
    key_order = jax.random.fold_in(key, 34)
    forced = jax.random.randint(key_forced, (), 0, devcount)
    rank = jax.random.permutation(key_rank, slots).astype(jnp.int32)
    owner = jnp.arange(slots, dtype=jnp.int32) // CAP
    rank = jnp.where(owner == forced, rank - slots, rank)
    order = jnp.argsort(rank, stable=True)[:MEDOIDS]
    row_keys = jax.random.split(key_rows, devcount)
    chosen = jax.vmap(lambda kk: jax.random.permutation(kk, ROWS_DEV))(row_keys)[:, :CAP]
    candid = jnp.arange(devcount, dtype=jnp.int32)[:, None] * ROWS_DEV + chosen.astype(jnp.int32)
    picked = candid.reshape(-1)[order]
    return picked[jax.random.permutation(key_order, MEDOIDS)].astype(jnp.int32)


def draw_weights(key, part):
    position = jnp.arange(POINTS, dtype=jnp.float32) / jnp.float32(max(POINTS - 1, 1))
    base = jnp.exp(jax.random.uniform(jax.random.fold_in(key, 22), (POINTS,), jnp.float32, -0.69, 0.69))
    ramp = 1.0 + 2.0 * position
    return (base * ramp).astype(jnp.float32)


def steps_of(own_key, extent, pieces, low, top_value):
    def one(dim, shards_of):
        steps = jax.random.uniform(jax.random.fold_in(jax.random.fold_in(own_key, 6), dim), (shards_of,), jnp.float32, low / len(pieces), top_value / len(pieces))
        return jnp.repeat(jnp.exp(steps), extent[dim] // shards_of).reshape((-1,) + (1,) * (len(extent) - dim - 1))

    factor_of = one(*pieces[0])
    for cut in pieces[1:]:
        factor_of = factor_of * one(*cut)
    return factor_of


def scatter_about(stream_key, shape, deviation, reach, pieces=(), kind=jnp.bfloat16):
    drawn = jax.random.normal(stream_key, shape, jnp.float32) * deviation
    if len(pieces) > 0:
        drawn = steps_of(stream_key, shape, pieces, -0.22, 0.18) * drawn
    return jnp.clip(drawn, min=-reach, max=reach).astype(kind)


def setup_inputs(seed: int = 0) -> dict:
    key_of = jax.random.split(jax.random.key(seed), 4)
    return {
        "points": scatter_about(key_of[0], (POINTS, D), 1.0, 6.0, ((0, 128),), jnp.float32),
        "weights": draw_weights(jax.random.fold_in(key_of[3], 71), 0),
        "medoid_ids": draw_medoid_ids(jax.random.fold_in(key_of[3], 71), 0),
    }


EPS = 1e-06

def reference(points, weights, medoid_ids):
    unit = points * lax.rsqrt(lax.optimization_barrier(jnp.sum(points * points, axis=1, keepdims=True)) + EPS)
    centers = jnp.take(unit, medoid_ids.astype(jnp.int32), axis=0)
    blocks = unit.reshape(POINTS // ROWS_DEV, ROWS_DEV, D)

    def block_cover(rows):
        sims = lax.dot_general(rows, centers, (((1,), (1,)), ((), ())), precision=lax.Precision.HIGHEST, preferred_element_type=jnp.float32)
        return lax.optimization_barrier(jnp.max(sims, axis=1))
    cover = lax.map(block_cover, blocks).reshape(POINTS)
    total = jnp.sum(weights * cover) / jnp.sum(weights)
    return (cover, total)
```

```python
import functools

import jax
import jax.numpy as jnp
from jax import lax
from jax.experimental import pallas as pl
from jax.experimental.pallas import tpu as pltpu
from jax.sharding import Mesh
from jax.sharding import PartitionSpec as P


AXES = ("pts_0", "pts_1", "med_0", "med_1", "med_2")
NATURAL = ("pts_0", "med_0", "pts_1", "med_1", "med_2")
SIDE = 4
CAP = 24
TILE = 256
BLOCK = 1024
SUB = 8
LANES = 128
STRIP = 32
EPS = 1e-06
LOW = -1.0e30
PHASES = ((0, 1), (1, 2), (2, 0))


def linear(x, y, z, c):
    return (((x // 2 * SIDE + y) * 2 + x % 2) * SIDE + z) * 2 + c


def moved(value, phase, step):
    pairs = []
    for x in range(SIDE):
        for y in range(SIDE):
            for z in range(SIDE):
                for c in range(2):
                    to = [x, y, z]
                    axis = PHASES[phase][c]
                    to[axis] = (to[axis] + step) % SIDE
                    pairs.append((linear(x, y, z, c), linear(*to, c)))
    return lax.ppermute(value, AXES, pairs)


def swapped(value):
    return lax.ppermute(value, "med_2", [(0, 1), (1, 0)])


def pick_kernel(device, ids, points, out, found, where, sems):
    local = ids[...] - device[0] * points.shape[0]
    owned = jnp.logical_and(local >= 0, local < points.shape[0])
    mark = owned.astype(jnp.float32)
    lanes = lax.broadcasted_iota(jnp.int32, (LANES, LANES), 0)
    before = (lanes < lax.broadcasted_iota(jnp.int32, (LANES, LANES), 1)).astype(jnp.float32)
    in_row = jnp.dot(mark, before, preferred_element_type=jnp.float32)
    tall = ids.shape[0]
    row = lax.broadcasted_iota(jnp.int32, (tall, tall), 0)
    above = (lax.broadcasted_iota(jnp.int32, (tall, tall), 1) < row).astype(jnp.float32)
    per_row = jnp.broadcast_to(jnp.sum(mark, axis=1, keepdims=True), mark.shape)
    rank = (in_row + jnp.dot(above, per_row, preferred_element_type=jnp.float32)).astype(jnp.int32)
    rank = jnp.where(owned, rank, -1)
    count = jnp.sum(mark).astype(jnp.int32)
    for k in range(CAP):
        where[k] = jnp.sum(jnp.where(rank == k, local, 0).astype(jnp.float32)).astype(jnp.int32)

    def copy(k):
        return pltpu.make_async_copy(
            points.at[pl.ds(where[k], 1)], found.at[pl.ds(k, 1)], sems.at[k]
        )

    for k in range(CAP):
        pl.when(k < count)(lambda k=k: copy(k).start())
    for k in range(CAP):
        pl.when(k < count)(lambda k=k: copy(k).wait())
    for j in range(SUB):
        out[pl.ds(j, CAP, stride=SUB), :] = found[:, j * LANES : (j + 1) * LANES]


def pick(points, medoid_ids, device):
    return pl.pallas_call(
        pick_kernel,
        name="pick_rows",
        out_shape=jax.ShapeDtypeStruct((CAP * SUB, LANES), points.dtype),
        in_specs=[
            pl.BlockSpec(memory_space=pltpu.SMEM),
            pl.BlockSpec(memory_space=pltpu.VMEM),
            pl.BlockSpec(memory_space=pltpu.HBM),
        ],
        out_specs=pl.BlockSpec(memory_space=pltpu.VMEM),
        scratch_shapes=[
            pltpu.VMEM((CAP, points.shape[1]), points.dtype),
            pltpu.SMEM((CAP,), jnp.int32),
            pltpu.SemaphoreType.DMA((CAP,)),
        ],
    )(device[None].astype(jnp.int32), medoid_ids.reshape(-1, LANES), points)


def unit_halves(rows):
    unit = rows * lax.rsqrt(jnp.sum(rows * rows, axis=1, keepdims=True) + EPS)
    high = unit.astype(jnp.bfloat16)
    return high, (unit - high.astype(jnp.float32)).astype(jnp.bfloat16)


def split_kernel(points, high, low):
    for r in range(0, points.shape[0], STRIP):
        here = slice(r, r + STRIP)
        high[here, :], low[here, :] = unit_halves(points[here, :])


def split(points):
    rows, width = points.shape
    spec = pl.BlockSpec((BLOCK, width), lambda i: (i, 0))
    half = jax.ShapeDtypeStruct((rows, width), jnp.bfloat16)
    return pl.pallas_call(
        split_kernel,
        name="split_points",
        grid=(rows // BLOCK,),
        in_specs=[spec],
        out_specs=[spec, spec],
        out_shape=[half, half],
        compiler_params=pltpu.CompilerParams(vmem_limit_bytes=20 << 20),
        cost_estimate=pl.CostEstimate(flops=9_000_000_000, bytes_accessed=16 << 20, transcendentals=0),
    )(points)


def inner(a, b):
    return lax.dot_general(a, b, (((1,), (1,)), ((), ())), preferred_element_type=jnp.float32)


def match_kernel(first, pieces, *refs):
    counts, refs = refs[0], refs[1:]
    parts, refs = refs[:pieces], refs[pieces:]
    high, low = refs[:2]
    best, packed, center_high, center_low = refs[-4:]

    if first:
        best[...] = jnp.full(best.shape, LOW, jnp.float32)
    offset = counts[0]
    done = offset // TILE
    slot = 1
    for part in parts:
        for b in range(0, part.shape[0], CAP * SUB):
            to = pl.multiple_of(offset * SUB, SUB)
            packed[pl.ds(to, CAP * SUB), :] = part[b : b + CAP * SUB, :]
            offset = offset + counts[slot]
            slot += 1
    full = offset // TILE

    def center(t):
        for r in range(0, TILE, STRIP):
            start = pl.multiple_of(t * TILE + r, STRIP)
            rows = jnp.concatenate(
                [packed[pl.ds(start * SUB + j, STRIP, stride=SUB), :] for j in range(SUB)], axis=1
            )
            here = pl.ds(pl.multiple_of((t - done) * TILE + r, STRIP), STRIP)
            center_high[here, :], center_low[here, :] = unit_halves(rows)

    def tile(t, _):
        center(t + 1)
        here = pl.ds(pl.multiple_of((t - done) * TILE, TILE), TILE)
        for r in range(0, high.shape[0], BLOCK):
            mine = slice(r, r + BLOCK)
            sims = inner(high[mine, :], center_high[here, :])
            sims += inner(low[mine, :], center_high[here, :])
            sims += inner(high[mine, :], center_low[here, :])
            best[mine, :] = jnp.maximum(
                best[mine, :], jnp.maximum(sims[:, :LANES], sims[:, LANES:])
            )
        return 0

    center(done)
    lax.fori_loop(done, full, tile, 0)


def match(parts, counts, high, low, state, total):
    rows, width = high.shape
    slots = sum(p.shape[0] for p in parts) // SUB
    most = (slots + TILE - 1) // TILE
    args = [counts, *parts, high, low, *(state or ())]
    whole = pl.BlockSpec(memory_space=pltpu.VMEM)
    room = total + TILE
    return pl.pallas_call(
        functools.partial(match_kernel, state is None, len(parts)),
        name="match_first" if state is None else "match_more",
        in_specs=[pl.BlockSpec(memory_space=pltpu.SMEM)] + [whole] * (len(args) - 1),
        out_specs=[whole, whole],
        out_shape=[
            jax.ShapeDtypeStruct((rows, LANES), jnp.float32),
            jax.ShapeDtypeStruct((room * SUB, LANES), jnp.float32),
        ],
        input_output_aliases={} if state is None else {len(args) - 2: 0, len(args) - 1: 1},
        scratch_shapes=[
            pltpu.VMEM(((most + 1) * TILE, width), jnp.bfloat16),
            pltpu.VMEM(((most + 1) * TILE, width), jnp.bfloat16),
        ],
        compiler_params=pltpu.CompilerParams(vmem_limit_bytes=14 << 20),
        cost_estimate=pl.CostEstimate(flops=13_000_000_000, bytes_accessed=16 << 20, transcendentals=0),
    )(*args)


def owners(steps, coords, core):
    s = jnp.asarray(steps, jnp.int32)
    own = jnp.bitwise_xor(core, s[:, 3])
    at = [jnp.broadcast_to(v, own.shape) for v in coords]
    for phase in range(3):
        for c in range(2):
            axis = PHASES[phase][c]
            at[axis] = jnp.where(own == c, (at[axis] - s[:, phase]) % SIDE, at[axis])
    return linear(*at, own)


def body(points, weights, medoid_ids):
    rows = points.shape[0]
    total = medoid_ids.shape[0]
    mine = pick(points, medoid_ids, lax.axis_index(AXES))

    line_steps = [(s,) for s in (0, 1, -1, 2)]
    early = [l + (0,) for l in line_steps]
    rest = [l + (s,) for s in (1, -1, 2) for l in line_steps]
    half = len(rest) // 2
    rest_a, rest_b = rest[:half], rest[half:]
    own, other = 0, 1
    groups = (
        [(early, 0, own), (rest, 0, own), (early, 0, other), (rest, 0, other),
         (early, 1, own), (early, -1, own)],
        [(rest_b, 1, own), (rest_a, -1, own), (early, 1, other), (early, -1, other),
         (rest_b, 1, other), (rest_a, -1, other)],
        [(rest_a, 1, own), (rest_b, -1, own), (early, 2, own),
         (rest_a, 1, other), (rest_b, -1, other), (early, 2, other)],
        [(rest_b, 2, own), (rest_a, 2, own), (rest_b, 2, other), (rest_a, 2, other)],
    )
    steps = [t + (s, c) for g in groups for p, s, c in g for t in p]
    coords = (
        lax.axis_index(("pts_0", "med_0")), lax.axis_index("pts_1"), lax.axis_index("med_1"),
    )
    owner = owners(steps, coords, lax.axis_index("med_2"))
    counts = jnp.sum((owner[:, None] == (medoid_ids // rows)[None, :]).astype(jnp.int32), axis=1)
    start = jnp.cumsum(counts) - counts
    tables, at = [], 0
    for g in groups:
        size = sum(len(p) for p, _, _ in g)
        tables.append(jnp.concatenate([start[at : at + 1], counts[at : at + size]]))
        at += size

    line = jnp.concatenate([mine, moved(mine, 0, 1), moved(mine, 0, -1), moved(mine, 0, 2)])
    line, points, tables = lax.optimization_barrier((line, points, tables))
    plane = [moved(line, 1, 1), moved(line, 1, -1), moved(line, 1, 2)]
    line_up, line_down, line_far = (moved(line, 2, 1), moved(line, 2, -1), moved(line, 2, 2))
    line_other = swapped(line)
    high, low = split(points)
    plane[2], high, low, line_other = lax.optimization_barrier((plane[2], high, low, line_other))
    rest = jnp.concatenate(plane)
    half = rest.shape[0] // 2
    a, b = rest[:half], rest[half:]
    up_b, down_a = moved(b, 2, 1), moved(a, 2, -1)
    rest_other = swapped(rest)
    a, b, rest_other = lax.optimization_barrier((a, b, rest_other))
    up_a, down_b = moved(a, 2, 1), moved(b, 2, -1)
    up_other, down_other, far_other = swapped(line_up), swapped(line_down), swapped(line_far)

    state = match([line, rest, line_other, rest_other, line_up, line_down], tables[0], high, low, None, total)
    up_b, down_a, state = lax.optimization_barrier((up_b, down_a, state))
    far_b, far_a = moved(up_b, 2, 1), moved(down_a, 2, -1)
    second = [up_b, down_a, up_other, down_other, swapped(up_b), swapped(down_a)]
    up_a, down_b, state = lax.optimization_barrier((up_a, down_b, state))
    third = [up_a, down_b, line_far, swapped(up_a), swapped(down_b), far_other]
    state = match(second, tables[1], high, low, state, total)
    far_b, far_a, state = lax.optimization_barrier((far_b, far_a, state))
    last = [far_b, far_a, swapped(far_b), swapped(far_a)]
    state = match(third, tables[2], high, low, state, total)
    best, _ = match(last, tables[3], high, low, state, total)
    cover = jnp.max(best, axis=1)
    sums = jnp.stack([weights * cover, weights]).reshape(2, -1, LANES).sum(axis=1)
    everyone = lax.all_to_all(
        jnp.broadcast_to(sums, (lax.axis_size(NATURAL), *sums.shape)),
        NATURAL, split_axis=0, concat_axis=0, tiled=True,
    )
    both = jnp.sum(everyone, axis=(0, 2))
    return cover, both[0] / both[1]


def solution(mesh):
    finer = Mesh(mesh.devices.reshape(2, 4, 2, 4, 2), AXES)
    return jax.shard_map(
        body,
        mesh=finer,
        in_specs=(P(AXES, None), P(AXES), P()),
        out_specs=(P(AXES), P()),
        check_vma=False,
    )
```
